8 devices in a mesh: dp: 2 (over y, z), tp: 4 (over x, core).
Axes of the slice: x: 2, y: 2, z: 1, core: 2. Of those that a mesh axis runs over, the one named last changes fastest.
Arguments:
- x: bfloat16 [2048, 4096], P(('dp', 'tp')), parts along dimension 0
- gain: bfloat16 [4096], replicated
- wq: bfloat16 [4096, 12288], P(None, 'tp')
- wk: bfloat16 [4096, 1024], P(None, 'tp')
- wv: bfloat16 [4096, 1024], P(None, 'tp')
- wo: bfloat16 [12288, 4096], P('tp')
Outputs:
- output: bfloat16 [2048, 4096], P(('dp', 'tp')), parts along dimension 0
There are 2 independent parts. The reference program is written for one: setup_inputs(seed, part) draws one part's arguments, and reference() takes and returns one part's arrays. A program takes and returns all parts, laid end to end along the dimension named above; an argument that names none is the same for every part.
All inputs are finite; a program needn't handle non-finite values.
Results may differ from the reference program's by a relative error of at most 0.012.
Values are sent between devices in bfloat16 or wider.
A program may use at most 2 GiB of HBM per device.

```python
import jax
import jax.numpy as jnp
from jax import lax

ROWS = 1024
D = 4096
HEADS = 96
KV_HEADS = 8
HEAD = 128
THETA = 10000


def setup_inputs(seed: int = 0, part: int = 0) -> dict:
    kx, kn, kq, kk, kv, ko = jax.random.split(jax.random.key(seed), 6)

    def weights(key, rows, columns):
        return jax.random.normal(key, (rows, columns), jnp.float32) * rows**-0.5

    drawn = {
        "x": jax.random.normal(jax.random.fold_in(kx, part), (ROWS, D), jnp.float32),
        "gain": 1 + 0.1 * jax.random.normal(kn, (D,), jnp.float32),
        "wq": 2 * weights(kq, D, HEADS * HEAD),
        "wk": 2 * weights(kk, D, KV_HEADS * HEAD),
        "wv": 4 * weights(kv, D, KV_HEADS * HEAD),
        "wo": weights(ko, HEADS * HEAD, D),
    }
    return {k: v.astype(jnp.bfloat16) for k, v in drawn.items()}


def normed(x, gain):
    wide = x.astype(jnp.float32)
    scale = lax.rsqrt(jnp.mean(wide * wide, -1, keepdims=True) + 1e-6)
    return (wide * scale * gain.astype(jnp.float32)).astype(jnp.bfloat16)


def turned(t, place, theta):
    half = t.shape[-1] // 2
    angle = place.astype(jnp.float32)[:, None] * theta ** (-jnp.arange(half, dtype=jnp.float32) / half)
    cos, sin = jnp.cos(angle)[:, None], jnp.sin(angle)[:, None]
    a, b = t[..., :half].astype(jnp.float32), t[..., half:].astype(jnp.float32)
    return jnp.concatenate([a * cos - b * sin, b * cos + a * sin], -1).astype(jnp.bfloat16)


def matmul(a, w):
    return jnp.dot(a, w, preferred_element_type=jnp.float32).astype(jnp.bfloat16)


def einsum(form, a, b):
    return jnp.einsum(form, a.astype(jnp.float32), b.astype(jnp.float32))


def attention(q, k, v):
    scores = einsum("tgsd,ugd->gstu", q, k) * q.shape[-1] ** -0.5
    token = jnp.arange(q.shape[0])
    scores = jnp.where(token[:, None] >= token, scores, -jnp.inf)
    weights = jax.nn.softmax(scores, -1).astype(jnp.bfloat16)
    return einsum("gstu,ugd->tgsd", weights, v).astype(jnp.bfloat16)


def reference(x, gain, wq, wk, wv, wo):
    a, place = normed(x, gain), jnp.arange(ROWS)
    q = turned(matmul(a, wq).reshape(ROWS, HEADS, HEAD), place, THETA).reshape(ROWS, KV_HEADS, -1, HEAD)
    k = turned(matmul(a, wk).reshape(ROWS, KV_HEADS, HEAD), place, THETA)
    v = matmul(a, wv).reshape(ROWS, KV_HEADS, HEAD)
    seen = attention(q, k, v).reshape(ROWS, HEADS * HEAD)
    return (x.astype(jnp.float32) + jnp.dot(seen, wo, preferred_element_type=jnp.float32)).astype(jnp.bfloat16)
```

```python
import jax
import jax.numpy as jnp
import numpy as np
from jax import lax
from jax.experimental import pallas as pl
from jax.experimental.pallas import tpu as pltpu
from jax.sharding import PartitionSpec as P

HEAD = 128
THETA = 10000
NEG = -1e30
HIDDEN = 2 * NEG
LOG2E = 1.4426950408889634
MESH = pl.DeviceIdType.MESH
BF, F32 = jnp.bfloat16, jnp.float32
VMEM = 63 * 2**20
TILE = 512
PART = TILE // 2
SLOTS = 4


def _dot(a, b, ca, cb):
    return lax.dot_general(a, b, (((ca,), (cb,)), ((), ())), preferred_element_type=F32)


def _at(start, size):
    return pl.ds(pl.multiple_of(start, size), size)


def _whole(x_ref, gain_ref, tab_ref, wq_ref, wk_ref, wv_ref, wo_ref, y_ref,
           a_s, cos_s, sin_s, q_s, k_s, vt_s, seen_s, acc_s, top_s, mix_s, w_s, part_s, dsend_s, drecv_s, xsend_s, xrecv_s,
           osend_s, orecv_s, own_s, w_sem, g_send, g_recv, d_send, d_recv, x_send, x_recv, o_send, o_recv):
    rows, width = x_ref.shape
    half, chunk, piece = 2 * rows, rows, rows // 2
    depth = wo_ref.shape[0]
    groups = k_s.shape[0]
    shared = q_s.shape[0] // groups
    per = TILE // HEAD
    nq, no = wq_ref.shape[1] // TILE, width // TILE
    np_, nc = 1 + nq, 1 + nq + no
    total = np_ + 2 * nc + no
    dp, tp = lax.axis_index("dp"), lax.axis_index("tp")
    chip, core = lax.div(tp, 2), lax.rem(tp, 2)
    partner = tp + 1 - 2 * core
    across = tp + 2 - 4 * chip
    diagonal = partner + 2 - 4 * chip
    own, other = half * chip, half - half * chip

    def fetch(i):
        i = jnp.asarray(i, jnp.int32)
        slot = lax.rem(i, SLOTS)
        k = jnp.where(i < np_, i, jnp.where(i < np_ + 2 * nc, lax.rem(i - np_, nc), i - 2 * nc))

        def put(ref, j, part):
            src = ref.at[:, _at(j * PART, PART)]
            pltpu.make_async_copy(src, w_s.at[slot, pl.ds(0, ref.shape[0]), pl.ds(part * PART, PART)], w_sem.at[slot, part]).start()

        @pl.when(k == 0)
        def _():
            put(wk_ref, 0, 0)
            put(wv_ref, 0, 1)

        @pl.when((k > 0) & (k < np_))
        def _():
            put(wq_ref, 2 * (k - 1), 0)
            put(wq_ref, 2 * (k - 1) + 1, 1)

        @pl.when((k >= np_) & (i < total))
        def _():
            put(wo_ref, 2 * (k - np_), 0)
            put(wo_ref, 2 * (k - np_) + 1, 1)

    def take(i, ref):
        slot = lax.rem(jnp.asarray(i, jnp.int32), SLOTS)
        for part in range(2):
            dst = w_s.at[slot, pl.ds(0, ref.shape[0]), pl.ds(part * PART, PART)]
            pltpu.make_async_copy(ref.at[:, pl.ds(0, PART)], dst, w_sem.at[slot, part]).wait()
        return slot

    for i in range(SLOTS):
        fetch(i)

    barrier = pltpu.get_barrier_semaphore()
    for device in (partner, across, diagonal):
        pl.semaphore_signal(barrier, inc=1, device_id=(dp, device), device_id_type=MESH)

    gain = gain_ref[...].astype(F32)

    def norm(first):
        def some(i, _):
            at = first + 16 * i
            wide = x_ref[_at(at, 16), :].astype(F32)
            scale = lax.rsqrt(jnp.mean(wide * wide, -1, keepdims=True) + 1e-6)
            a_s[_at(own + rows * core + at, 16), :] = (wide * scale * gain).astype(BF)

        lax.fori_loop(0, piece // 16, some, None)

    def gather(k, first, count, device):
        ref = a_s.at[_at(first, count)]
        return pltpu.make_async_remote_copy(ref, ref, g_send.at[k], g_recv.at[k], device_id=(dp, device), device_id_type=MESH)

    urgent, later = piece * (1 - core), piece * core
    norm(urgent)
    pl.semaphore_wait(barrier, 3)
    mine, theirs = own + rows * core, own + rows * (1 - core)
    gather(0, mine + urgent, piece, partner).start()
    norm(later)
    gather(1, mine + later, piece, partner).start()
    gather(0, theirs + later, piece, partner).wait_recv()
    for p in range(2):
        gather(2 + p, own + chunk * p + piece * core, piece, across).start()

    tab = tab_ref[...]
    low = lax.broadcasted_iota(jnp.int32, tab.shape, 1) < HEAD // 2
    swapped = pltpu.roll(tab, HEAD // 2, 1)
    cos_s[...] = jnp.where(low, tab, swapped)
    sin_s[...] = jnp.where(low, -swapped, tab)
    vt_s[:, HEAD:, :] = jnp.ones((groups, vt_s.shape[1] - HEAD, vt_s.shape[2]), BF)

    gather(1, theirs + urgent, piece, partner).wait_recv()

    def turned(t, at):
        t = t.astype(BF).astype(F32)
        return (t * cos_s[at, :] + pltpu.roll(t, HEAD // 2, 1) * sin_s[at, :]).astype(BF)

    def project(place, held, m, first):
        at = _at(place, m)
        slot = take(first, wq_ref)
        acc_s[pl.ds(0, m)] = _dot(a_s[at, :], w_s[slot], 1, 0)
        fetch(first + SLOTS)
        for g in range(groups):
            k_s[g, at, :] = turned(acc_s[pl.ds(0, m), pl.ds(g * HEAD, HEAD)], at)
            vt_s[g, pl.ds(0, HEAD), at] = acc_s[pl.ds(0, m), pl.ds(PART + g * HEAD, HEAD)].T.astype(BF)

        def tile(n, _):
            slot = take(first + 1 + n, wq_ref)
            acc_s[pl.ds(0, m)] = _dot(a_s[at, :], w_s[slot], 1, 0)
            fetch(first + 1 + n + SLOTS)
            for h in range(per):
                q_s[per * n + h, _at(held, m), :] = turned(acc_s[pl.ds(0, m), pl.ds(h * HEAD, HEAD)], at)

        lax.fori_loop(0, nq, tile, None)

    e = HEAD**-0.5 * LOG2E
    wide = 2 * chunk
    strips = shared // 2

    def attention(place, held, seen):
        whole = lax.div(place, chunk)

        def group(g, _):
            top_s[...] = jnp.full(top_s.shape, NEG, F32)
            mix_s[...] = jnp.zeros(mix_s.shape, F32)

            def block(j, masked):
                here = _at(j * chunk, chunk)
                keys, values = k_s[g, here, :], vt_s[g, :, here]
                scores = [_dot(keys, q_s[pl.ds(g * shared + 2 * i, 2), _at(held, chunk), :].reshape(wide, HEAD), 1, 1) for i in range(strips)]
                if masked:
                    query = lax.rem(lax.broadcasted_iota(jnp.int32, (chunk, wide), 1), chunk)
                    ok = query >= lax.broadcasted_iota(jnp.int32, (chunk, wide), 0)
                weights, keeps = [], []
                for i, s in enumerate(scores):
                    if masked:
                        s = jnp.where(ok, s, HIDDEN)
                    old = top_s[:, pl.ds(i * wide, wide)]
                    top = jnp.maximum(old, s.max(axis=0, keepdims=True))
                    top_s[:, pl.ds(i * wide, wide)] = top
                    weights.append(jnp.exp2((s - top) * e).astype(BF))
                    keeps.append(jnp.exp2((old - top) * e))
                for i, (w, keep) in enumerate(zip(weights, keeps)):
                    mix_s[:, pl.ds(i * wide, wide)] = mix_s[:, pl.ds(i * wide, wide)] * keep + _dot(values, w, 1, 0)

            lax.fori_loop(0, whole, lambda j, _: block(j, False), None)
            block(whole, True)
            for n in range(shared):
                cols = pl.ds(n * chunk, chunk)
                out = mix_s[pl.ds(0, HEAD), cols] * (1 / mix_s[pl.ds(HEAD, 1), cols])
                seen_s[_at(seen, chunk), _at((g * shared + n) * HEAD, HEAD)] = out.T.astype(BF)

        lax.fori_loop(0, groups, group, None)

    def pair(p, n):
        return pltpu.make_async_remote_copy(dsend_s.at[p, n], drecv_s.at[p, n], d_send.at[p, n], d_recv.at[p, n],
                                            device_id=(dp, partner), device_id_type=MESH)

    def link(p, n, source, device):
        return pltpu.make_async_remote_copy(xsend_s.at[p, n], xrecv_s.at[source, n], x_send.at[p, n], x_recv.at[source, n],
                                            device_id=(dp, device), device_id_type=MESH)

    def swap(n):
        return pltpu.make_async_remote_copy(osend_s.at[n], orecv_s.at[n], o_send.at[n], o_recv.at[n], device_id=(dp, partner), device_id_type=MESH)

    project(own, 0, half, 0)

    def arrived(p, _):
        place = other + chunk * p
        first = np_ + nc * p
        gather(2 + p, place + piece * core, piece, across).wait_recv()
        gather(4 + p, place + piece * core, piece, partner).start()
        gather(4 + p, place + piece * (1 - core), piece, partner).wait_recv()
        project(place, half, chunk, first)
        attention(place, half, 0)

        def add(n):
            pair(p, n).wait_recv()
            xsend_s[p, n] = (part_s[lax.rem(n, 2)] + drecv_s[p, n].astype(F32)).astype(BF)
            link(p, n, core, 2 * (1 - chip) + p).start()

        def tile(n, _):
            slot = take(first + np_ + n, wo_ref)
            acc_s[pl.ds(0, chunk)] = _dot(seen_s[pl.ds(0, chunk)], w_s[slot, pl.ds(0, depth)], 1, 0)
            fetch(first + np_ + n + SLOTS)
            dsend_s[p, n] = acc_s[_at(piece * (1 - core), piece)].astype(BF)
            pair(p, n).start()
            part_s[lax.rem(n, 2)] = acc_s[_at(piece * core, piece)]
            pl.when(n > 0)(lambda: add(n - 1))

        lax.fori_loop(0, no, tile, None)
        add(jnp.int32(no - 1))

    lax.fori_loop(0, 2, arrived, None)
    lax.fori_loop(0, 2, lambda i, _: attention(own + chunk * i, chunk * i, chunk * i), None)

    def last(n, _):
        slot = take(np_ + 2 * nc + n, wo_ref)
        acc_s[...] = _dot(seen_s[...], w_s[slot, pl.ds(0, depth)], 1, 0)
        fetch(np_ + 2 * nc + n + SLOTS)
        osend_s[n] = acc_s[_at(rows * (1 - core), rows)].astype(BF)
        swap(n).start()
        own_s[n] = acc_s[_at(rows * core, rows)]

    lax.fori_loop(0, no, last, None)

    def finish(n, _):
        swap(n).wait_recv()
        for source in range(2):
            link(0, n, source, across).wait_recv()
        cols = _at(n * TILE, TILE)
        for source in range(2):
            at = pl.ds(source * piece, piece)
            summed = own_s[n, at] + orecv_s[n, at].astype(F32) + xrecv_s[source, n].astype(F32)
            y_ref[at, cols] = (x_ref[at, cols].astype(F32) + summed).astype(BF)

    lax.fori_loop(0, no, finish, None)

    gather(0, mine + urgent, piece, partner).wait_send()
    gather(1, mine + later, piece, partner).wait_send()
    for p in range(2):
        gather(2 + p, own + chunk * p + piece * core, piece, across).wait_send()
        gather(4 + p, other + chunk * p + piece * core, piece, partner).wait_send()

    def sent(n, _):
        for p in range(2):
            pair(p, n).wait_send()
            link(p, n, core, across).wait_send()
        swap(n).wait_send()

    lax.fori_loop(0, no, sent, None)


def _table(tokens):
    half = HEAD // 2
    power = np.float32(THETA) ** (-np.arange(half, dtype=np.float32) / np.float32(half))
    angle = np.arange(tokens, dtype=np.float32)[:, None] * power.astype(np.float32)
    return np.concatenate([np.cos(angle), np.sin(angle)], 1).astype(np.float32)


def solution(mesh):
    group = mesh.shape["tp"]

    def step(x, gain, wq, wk, wv, wo):
        rows, width = x.shape
        tokens, piece = rows * group, rows // 2
        heads, groups = wq.shape[1] // HEAD, wk.shape[1] // HEAD
        depth, no = wo.shape[0], width // TILE
        dma = pltpu.SemaphoreType.DMA
        vmem, hbm = pl.BlockSpec(memory_space=pltpu.VMEM), pl.BlockSpec(memory_space=pltpu.HBM)
        cols = heads // groups * rows
        return pl.pallas_call(
            _whole,
            out_shape=jax.ShapeDtypeStruct((rows, width), BF),
            in_specs=[vmem, vmem, vmem, hbm, hbm, hbm, hbm],
            out_specs=vmem,
            scratch_shapes=[
                pltpu.VMEM((tokens, width), BF),
                pltpu.VMEM((tokens, HEAD), F32),
                pltpu.VMEM((tokens, HEAD), F32),
                pltpu.VMEM((heads, 3 * rows, HEAD), BF),
                pltpu.VMEM((groups, tokens, HEAD), BF),
                pltpu.VMEM((groups, HEAD + 16, tokens), BF),
                pltpu.VMEM((2 * rows, depth), BF),
                pltpu.VMEM((2 * rows, TILE), F32),
                pltpu.VMEM((1, cols), F32),
                pltpu.VMEM((HEAD + 16, cols), F32),
                pltpu.VMEM((SLOTS, width, TILE), BF),
                pltpu.VMEM((2, piece, TILE), F32),
                pltpu.VMEM((2, no, piece, TILE), BF),
                pltpu.VMEM((2, no, piece, TILE), BF),
                pltpu.VMEM((2, no, piece, TILE), BF),
                pltpu.VMEM((2, no, piece, TILE), BF),
                pltpu.VMEM((no, rows, TILE), BF),
                pltpu.VMEM((no, rows, TILE), BF),
                pltpu.VMEM((no, rows, TILE), F32),
                dma((SLOTS, 2)), dma((6,)), dma((6,)), dma((2, no)), dma((2, no)), dma((2, no)), dma((2, no)), dma((no,)), dma((no,)),
            ],
            compiler_params=pltpu.CompilerParams(collective_id=0, has_side_effects=True, vmem_limit_bytes=VMEM),
            cost_estimate=pl.CostEstimate(flops=2 * tokens * width * (2 * depth + 2 * groups * HEAD) + 2 * heads * tokens * tokens * HEAD,
                                          transcendentals=heads * tokens * tokens // 2,
                                          bytes_accessed=3 * 2 * width * (2 * depth + 2 * groups * HEAD)),
        )(x, gain.reshape(1, width), jnp.asarray(_table(tokens)), wq, wk, wv, wo)

    tokens, columns = P(("dp", "tp"), None), P(None, "tp")
    return jax.shard_map(
        step,
        mesh=mesh,
        in_specs=(tokens, P(None), columns, columns, columns, P("tp", None)),
        out_specs=tokens,
        check_vma=False,
    )
```

```python
import jax
import jax.numpy as jnp
import numpy as np
from jax import lax
from jax.experimental import pallas as pl
from jax.experimental.pallas import tpu as pltpu
from jax.sharding import PartitionSpec as P

HEAD = 128
THETA = 10000
NEG = -1e30
HIDDEN = 2 * NEG
LOG2E = 1.4426950408889634
MESH = pl.DeviceIdType.MESH
BF, F32 = jnp.bfloat16, jnp.float32
VMEM = 67_043_328
TILE = 512
PART = TILE // 2
SLOTS = 4


def _dot(a, b, ca, cb):
    return lax.dot_general(a, b, (((ca,), (cb,)), ((), ())), preferred_element_type=F32)


def _at(start, size):
    return pl.ds(pl.multiple_of(start, size), size)


def _whole(x_ref, gain_ref, tab_ref, wq_ref, wk_ref, wv_ref, wo_ref, y_ref,
           gain_s, a_s, cos_s, sin_s, q_s, k_s, vt_s, seen_s, acc_s, top_s, mix_s, w_s, part_s, dsend_s, drecv_s, xrecv_s,
           w_sem, io_sem, g_send, g_recv, d_send, d_recv, x_send, x_recv, o_send, o_recv):
    rows, width = x_ref.shape
    half, chunk, piece = 2 * rows, rows, rows // 2
    depth = wo_ref.shape[0]
    groups = k_s.shape[0]
    shared = q_s.shape[0] // groups
    per = TILE // HEAD
    nq, no = wq_ref.shape[1] // TILE, width // TILE
    steps = no // 2
    np_, nc = 1 + nq, 1 + nq + no
    total = np_ + 2 * nc + no
    dp, tp = lax.axis_index("dp"), lax.axis_index("tp")
    chip, core = lax.div(tp, 2), lax.rem(tp, 2)
    partner = tp + 1 - 2 * core
    across = tp + 2 - 4 * chip
    diagonal = partner + 2 - 4 * chip
    own, other = half * chip, half - half * chip

    def fetch(i):
        i = jnp.asarray(i, jnp.int32)
        slot = lax.rem(i, SLOTS)
        k = jnp.where(i < np_, i, jnp.where(i < np_ + 2 * nc, lax.rem(i - np_, nc), i - 2 * nc))

        def put(ref, j, part):
            src = ref.at[:, _at(j * PART, PART)]
            pltpu.make_async_copy(src, w_s.at[slot, pl.ds(0, ref.shape[0]), pl.ds(part * PART, PART)], w_sem.at[slot, part]).start()

        @pl.when(k == 0)
        def _():
            put(wk_ref, 0, 0)
            put(wv_ref, 0, 1)

        @pl.when((k > 0) & (k < np_))
        def _():
            put(wq_ref, 2 * (k - 1), 0)
            put(wq_ref, 2 * (k - 1) + 1, 1)

        @pl.when((k >= np_) & (i < total))
        def _():
            put(wo_ref, 2 * (k - np_), 0)
            put(wo_ref, 2 * (k - np_) + 1, 1)

    def take(i, ref):
        slot = lax.rem(jnp.asarray(i, jnp.int32), SLOTS)
        for part in range(2):
            dst = w_s.at[slot, pl.ds(0, ref.shape[0]), pl.ds(part * PART, PART)]
            pltpu.make_async_copy(ref.at[:, pl.ds(0, PART)], dst, w_sem.at[slot, part]).wait()
        return slot

    def load(h):
        return pltpu.make_async_copy(x_ref.at[pl.ds(piece * h, piece)], a_s.at[_at(own + rows * core + piece * h, piece)], io_sem.at[h])

    load(0).start()
    load(1).start()
    table = pltpu.make_async_copy(tab_ref, sin_s, io_sem.at[2 + steps])
    table.start()
    barrier = pltpu.get_barrier_semaphore()
    for device in (partner, across, diagonal):
        pl.semaphore_signal(barrier, inc=1, device_id=(dp, device), device_id_type=MESH)

    for j in range(width // HEAD):
        gain_s[:, pl.ds(j * HEAD, HEAD)] = gain_ref[pl.ds(j, 1), :].astype(F32)
    gain = gain_s[...]

    def norm(h):
        def some(i, _):
            at = _at(own + rows * core + piece * h + 32 * i, 32)
            wide = a_s[at, :].astype(F32)
            scale = lax.rsqrt(jnp.mean(wide * wide, -1, keepdims=True) + 1e-6)
            a_s[at, :] = (wide * scale * gain).astype(BF)

        lax.fori_loop(0, piece // 32, some, None)

    def gather(k, first, device):
        ref = a_s.at[_at(first, piece)]
        return pltpu.make_async_remote_copy(ref, ref, g_send.at[k], g_recv.at[k], device_id=(dp, device), device_id_type=MESH)

    mine, theirs = own + rows * core, own + rows * (1 - core)

    def near(h, block=mine):
        return gather(h, block + piece * h, partner)

    def cross(h, block=mine):
        return gather(2 + h, block + piece * h, across)

    def relay(h, p):
        return gather(4 + h, other + chunk * p + piece * h, partner)

    def arrival(p, h):
        @pl.when(core == p)
        def _():
            cross(h, other + chunk * p).wait_recv()
            relay(h, p).start()

    for h in range(2):
        load(h).wait()
        norm(h)
        if h == 0:
            pl.semaphore_wait(barrier, 3)
        near(h).start()
        pl.when(core == 0)(cross(h).start)
        if h == 0:
            for i in range(SLOTS):
                fetch(i)

    table.wait()
    tab = sin_s[...]
    low = lax.broadcasted_iota(jnp.int32, tab.shape, 1) < HEAD // 2
    swapped = pltpu.roll(tab, HEAD // 2, 1)
    cos_s[...] = jnp.where(low, tab, swapped)
    sin_s[...] = jnp.where(low, -swapped, tab)
    vt_s[:, HEAD:, :] = jnp.ones((groups, vt_s.shape[1] - HEAD, vt_s.shape[2]), BF)

    def turned(t, at):
        t = t.astype(BF).astype(F32)
        return (t * cos_s[at, :] + pltpu.roll(t, HEAD // 2, 1) * sin_s[at, :]).astype(BF)

    def keys_values(slot, place):
        at = _at(place, chunk)
        acc_s[0, pl.ds(0, chunk)] = _dot(a_s[at, :], w_s[slot], 1, 0)
        for g in range(groups):
            k_s[g, at, :] = turned(acc_s[0, pl.ds(0, chunk), pl.ds(g * HEAD, HEAD)], at)
            vt_s[g, pl.ds(0, HEAD), at] = acc_s[0, pl.ds(0, chunk), pl.ds(PART + g * HEAD, HEAD)].T.astype(BF)

    def queries(place, held, m, first):
        at = _at(place, m)

        def tile(n, _):
            slots = [take(first + 2 * n + b, wq_ref) for b in range(2)]
            for b in range(2):
                acc_s[b, pl.ds(0, m)] = _dot(a_s[at, :], w_s[slots[b]], 1, 0)
                fetch(first + 2 * n + b + SLOTS)
            for b in range(2):
                for h in range(per):
                    q_s[per * (2 * n + b) + h, _at(held, m), :] = turned(acc_s[b, pl.ds(0, m), pl.ds(h * HEAD, HEAD)], at)

        lax.fori_loop(0, nq // 2, tile, None)

    e = HEAD**-0.5 * LOG2E
    wide = 2 * chunk
    strips = shared // 2

    parts = [(g, i) for g in range(groups) for i in range(strips)]

    def begin(b):
        for g in range(groups):
            top_s[b, g] = jnp.full(top_s.shape[2:], NEG, F32)
            mix_s[b, g] = jnp.zeros(mix_s.shape[2:], F32)

    def block(b, held, j, masked):
        here = _at(j * chunk, chunk)
        scores = [_dot(k_s[g, here, :], q_s[pl.ds(g * shared + 2 * i, 2), _at(held, chunk), :].reshape(wide, HEAD), 1, 1) for g, i in parts]
        if masked:
            query = lax.rem(lax.broadcasted_iota(jnp.int32, (chunk, wide), 1), chunk)
            ok = query >= lax.broadcasted_iota(jnp.int32, (chunk, wide), 0)
        weights, keeps = [], []
        for (g, i), s in zip(parts, scores):
            if masked:
                s = jnp.where(ok, s, HIDDEN)
            cols = pl.ds(i * wide, wide)
            old = top_s[b, g, :, cols]
            top = jnp.maximum(old, s.max(axis=0, keepdims=True))
            top_s[b, g, :, cols] = top
            weights.append(jnp.exp2((s - top) * e).astype(BF))
            keeps.append(jnp.exp2((old - top) * e))
        for (g, i), w, keep in zip(parts, weights, keeps):
            cols = pl.ds(i * wide, wide)
            mix_s[b, g, :, cols] = mix_s[b, g, :, cols] * keep + _dot(vt_s[g, :, here], w, 1, 0)

    def finish(b, seen):
        for k in range(groups * shared):
            g, cols = k // shared, pl.ds(k % shared * chunk, chunk)
            out = mix_s[b, g, pl.ds(0, HEAD), cols] * (1 / mix_s[b, g, pl.ds(HEAD, 1), cols])
            seen_s[_at(seen, chunk), pl.ds(k * HEAD, HEAD)] = out.T.astype(BF)

    def pair(p, n):
        return pltpu.make_async_remote_copy(dsend_s.at[n, pl.ds(p * piece, piece)], drecv_s.at[p, n], d_send.at[p, n], d_recv.at[p, n],
                                            device_id=(dp, partner), device_id_type=MESH)

    def link(p, n, source, device):
        return pltpu.make_async_remote_copy(drecv_s.at[p, n], xrecv_s.at[source, n], x_send.at[p, n], x_recv.at[source, n],
                                            device_id=(dp, device), device_id_type=MESH)

    def swap(n):
        dst = a_s.at[pl.ds(0, rows), _at(n * 2 * TILE, 2 * TILE)]
        return pltpu.make_async_remote_copy(dsend_s.at[n], dst, o_send.at[n], o_recv.at[n], device_id=(dp, partner), device_id_type=MESH)

    slot = take(0, wq_ref)

    def local(i, _):
        @pl.when(i == 1)
        def _():
            for h in range(2):
                near(h, theirs).wait_recv()

        keys_values(slot, jnp.where(i == 0, mine, theirs))

    lax.fori_loop(0, 2, local, None)
    fetch(SLOTS)
    queries(own, 0, half, 1)
    arrival(0, 0)

    def inner(i, _):
        begin(i)
        first = lax.div(own, chunk)
        lax.fori_loop(0, i, lambda j, _: block(i, i * chunk, first + j, False), None)

        @pl.when((i == 1) & (core == 1))
        def _():
            for h in range(2):
                cross(h).start()

        pl.when(i == 1)(lambda: arrival(0, 1))
        block(i, i * chunk, first + i, True)


    lax.fori_loop(0, 2, inner, None)

    def add(p, n):
        pair(p, n).wait_recv()
        drecv_s[p, n] = (part_s[lax.rem(n, 2)] + drecv_s[p, n].astype(F32)).astype(BF)

    def send(p, n):
        link(p, n, core, 2 * (1 - chip) + p).start()

    def arrived(p, _):
        place = other + chunk * p
        first = np_ + nc * p

        @pl.when(core != p)
        def _():
            for h in range(2):
                relay(h, p).wait_recv()

        slot = take(first, wq_ref)
        keys_values(slot, place)
        fetch(first + SLOTS)
        queries(place, half, chunk, first + 1)
        whole = lax.div(place, chunk)

        begin(2)
        lax.fori_loop(0, whole, lambda j, _: block(2, half, j, False), None)
        block(2, half, whole, True)
        finish(2, jnp.int32(0))

        @pl.when(p == 1)
        def _():
            add(p - 1, jnp.int32(steps - 1))
            send(p - 1, jnp.int32(steps - 1))
            for h in range(2):
                near(h).wait_send()
                cross(h).wait_send()
                relay(h, core).wait_send()

        def tile(n, _):
            slots = [take(first + np_ + 2 * n + b, wo_ref) for b in range(2)]
            pl.when((p == 0) & (n == 0))(lambda: arrival(1, 0))

            @pl.when((p == 0) & (n == steps - 1))
            def _():
                arrival(1, 1)
                for m in range(steps - 2):
                    send(p, jnp.int32(m))

            for b in range(2):
                acc_s[b, pl.ds(0, chunk)] = _dot(seen_s[pl.ds(0, chunk)], w_s[slots[b], pl.ds(0, depth)], 1, 0)
                fetch(first + np_ + 2 * n + b + SLOTS)
            for b in range(2):
                cols = pl.ds(b * TILE, TILE)
                dsend_s[n, _at(p * piece, piece), cols] = acc_s[b, _at(piece * (1 - core), piece)].astype(BF)
                part_s[lax.rem(n, 2), :, cols] = acc_s[b, _at(piece * core, piece)]
            pair(p, n).start()
            pl.when(n > 0)(lambda: add(p, n - 1))
            pl.when((n > 0) & ((p == 1) | (n == steps - 1)))(lambda: send(p, n - 1))

            def outer(i, _):
                block(i, i * chunk, p, False)

            lax.fori_loop(0, jnp.where((chip == 1) & (n == 1), 2, 0), outer, None)

        lax.fori_loop(0, steps, tile, None)

    lax.fori_loop(0, 2, arrived, None)

    lax.fori_loop(0, 2, lambda i, _: finish(i, i * chunk), None)
    add(1, jnp.int32(steps - 1))
    send(1, jnp.int32(steps - 1))
    wides = mix_s.shape[3] // TILE

    def kept(n, b, h):
        k = (2 * n + b) * 2 + h
        s = lax.div(k, wides)
        return lax.div(s, groups), lax.rem(s, groups), pl.ds(0, piece), _at(lax.rem(k, wides) * TILE, TILE)

    again = pltpu.make_async_copy(x_ref, a_s.at[pl.ds(rows, rows)], io_sem.at[0])
    again.start()

    def last(n, _):
        first = np_ + 2 * nc + 2 * n
        slots = [take(first + b, wo_ref) for b in range(2)]
        for p in range(2):
            pair(p, n).wait_send()
        for b in range(2):
            acc_s[b] = _dot(seen_s[...], w_s[slots[b], pl.ds(0, depth)], 1, 0)
        for b in range(2):
            dsend_s[n, :, pl.ds(b * TILE, TILE)] = acc_s[b, _at(rows * (1 - core), rows)].astype(BF)
            for h in range(2):
                mix_s[kept(n, b, h)] = acc_s[b, _at(rows * core + piece * h, piece)]
        swap(n).start()
        for b in range(2):
            fetch(first + b + SLOTS)

    lax.fori_loop(0, steps, last, None)

    def store(n):
        cols = _at(n * 2 * TILE, 2 * TILE)
        return pltpu.make_async_copy(a_s.at[pl.ds(rows, rows), cols], y_ref.at[:, cols], io_sem.at[2 + n])

    def close(n, _):
        swap(n).wait_recv()
        for source in range(2):
            link(0, n, source, across).wait_recv()
        for b in range(2):
            cols = _at((2 * n + b) * TILE, TILE)
            for source in range(2):
                at = pl.ds(source * piece, piece)
                summed = mix_s[kept(n, b, source)] + a_s[at, cols].astype(F32) + xrecv_s[source, n, :, pl.ds(b * TILE, TILE)].astype(F32)
                to = pl.ds(rows + source * piece, piece)
                a_s[to, cols] = (a_s[to, cols].astype(F32) + summed).astype(BF)
        store(n).start()

    again.wait()
    lax.fori_loop(0, steps, close, None)

    def sent(n, _):
        for p in range(2):
            link(p, n, core, across).wait_send()
        swap(n).wait_send()
        store(n).wait()

    lax.fori_loop(0, steps, sent, None)


def _table(tokens):
    half = HEAD // 2
    power = np.float32(THETA) ** (-np.arange(half, dtype=np.float32) / np.float32(half))
    angle = np.arange(tokens, dtype=np.float32)[:, None] * power.astype(np.float32)
    return np.concatenate([np.cos(angle), np.sin(angle)], 1).astype(np.float32)


def solution(mesh):
    group = mesh.shape["tp"]

    def step(x, gain, wq, wk, wv, wo):
        rows, width = x.shape
        tokens, piece = rows * group, rows // 2
        heads, groups = wq.shape[1] // HEAD, wk.shape[1] // HEAD
        depth, steps = wo.shape[0], width // TILE // 2
        dma = pltpu.SemaphoreType.DMA
        vmem, hbm = pl.BlockSpec(memory_space=pltpu.VMEM), pl.BlockSpec(memory_space=pltpu.HBM)
        cols = heads // groups * rows
        return pl.pallas_call(
            _whole,
            out_shape=jax.ShapeDtypeStruct((rows, width), BF),
            in_specs=[hbm, vmem, hbm, hbm, hbm, hbm, hbm],
            out_specs=hbm,
            scratch_shapes=[
                pltpu.VMEM((1, width), F32),
                pltpu.VMEM((tokens, width), BF),
                pltpu.VMEM((tokens, HEAD), F32),
                pltpu.VMEM((tokens, HEAD), F32),
                pltpu.VMEM((heads, 3 * rows, HEAD), BF),
                pltpu.VMEM((groups, tokens, HEAD), BF),
                pltpu.VMEM((groups, HEAD + 8, tokens), BF),
                pltpu.VMEM((2 * rows, depth), BF),
                pltpu.VMEM((2, 2 * rows, TILE), F32),
                pltpu.VMEM((3, groups, 1, cols), F32),
                pltpu.VMEM((3, groups, HEAD + 8, cols), F32),
                pltpu.VMEM((SLOTS, width, TILE), BF),
                pltpu.VMEM((2, piece, 2 * TILE), F32),
                pltpu.VMEM((steps, rows, 2 * TILE), BF),
                pltpu.VMEM((2, steps, piece, 2 * TILE), BF),
                pltpu.VMEM((2, steps, piece, 2 * TILE), BF),
                dma((SLOTS, 2)), dma((3 + steps,)), dma((6,)), dma((6,)), dma((2, steps)), dma((2, steps)), dma((2, steps)), dma((2, steps)),
                dma((steps,)), dma((steps,)),
            ],
            compiler_params=pltpu.CompilerParams(collective_id=0, has_side_effects=True, vmem_limit_bytes=VMEM),
            cost_estimate=pl.CostEstimate(flops=2 * tokens * width * (2 * depth + 2 * groups * HEAD) + 2 * heads * tokens * tokens * HEAD,
                                          transcendentals=heads * tokens * tokens // 2,
                                          bytes_accessed=3 * 2 * width * (2 * depth + 2 * groups * HEAD)),
        )(x, gain.reshape(width // HEAD, HEAD), jnp.asarray(_table(tokens)), wq, wk, wv, wo)

    tokens, columns = P(("dp", "tp"), None), P(None, "tp")
    return jax.shard_map(
        step,
        mesh=mesh,
        in_specs=(tokens, P(None), columns, columns, columns, P("tp", None)),
        out_specs=tokens,
        check_vma=False,
    )
```

```python
import jax
import jax.numpy as jnp
import numpy as np
from jax import lax
from jax.experimental import pallas as pl
from jax.experimental.pallas import tpu as pltpu
from jax.sharding import PartitionSpec as P

HEAD = 128
THETA = 10000
HIDDEN = -2e30
LOG2E = 1.4426950408889634
MESH = pl.DeviceIdType.MESH
BF, F32 = jnp.bfloat16, jnp.float32
VMEM = 67_043_328
TILE = 512
PART = TILE // 2
SLOTS = 4


def _dot(a, b, ca, cb):
    return lax.dot_general(a, b, (((ca,), (cb,)), ((), ())), preferred_element_type=F32)


def _at(start, size):
    return pl.ds(pl.multiple_of(start, size), size)


def _whole(x_ref, gain_ref, tab_ref, wq_ref, wk_ref, wv_ref, wo_ref, y_ref,
           gain_s, a_s, cos_s, sin_s, q_s, k_s, vt_s, seen_s, acc_s, top_s, mix_s, w_s, part_s, dsend_s, drecv_s, xrecv_s,
           w_sem, io_sem, g_send, g_recv, d_send, d_recv, x_send, x_recv, o_send, o_recv):
    rows, width = x_ref.shape
    half, chunk, piece = 2 * rows, rows, rows // 2
    depth = wo_ref.shape[0]
    groups = k_s.shape[0]
    shared = q_s.shape[0] // groups
    per = TILE // HEAD
    nq, no = wq_ref.shape[1] // TILE, width // TILE
    steps = no // 2
    np_, nc = 1 + nq, 1 + nq + no
    total = np_ + 2 * nc + no
    dp, tp = lax.axis_index("dp"), lax.axis_index("tp")
    chip, core = lax.div(tp, 2), lax.rem(tp, 2)
    partner = tp + 1 - 2 * core
    across = tp + 2 - 4 * chip
    diagonal = partner + 2 - 4 * chip
    own, other = half * chip, half - half * chip

    def fetch(i):
        i = jnp.asarray(i, jnp.int32)
        slot = lax.rem(i, SLOTS)
        k = jnp.where(i < np_, i, jnp.where(i < np_ + 2 * nc, lax.rem(i - np_, nc), i - 2 * nc))

        def put(ref, j, part):
            src = ref.at[:, _at(j * PART, PART)]
            pltpu.make_async_copy(src, w_s.at[slot, pl.ds(0, ref.shape[0]), pl.ds(part * PART, PART)], w_sem.at[slot, part]).start()

        @pl.when(k == 0)
        def _():
            put(wk_ref, 0, 0)
            put(wv_ref, 0, 1)

        @pl.when((k > 0) & (k < np_))
        def _():
            put(wq_ref, 2 * (k - 1), 0)
            put(wq_ref, 2 * (k - 1) + 1, 1)

        @pl.when((k >= np_) & (i < total))
        def _():
            put(wo_ref, 2 * (k - np_), 0)
            put(wo_ref, 2 * (k - np_) + 1, 1)

    def take(i, ref):
        slot = lax.rem(jnp.asarray(i, jnp.int32), SLOTS)
        for part in range(2):
            dst = w_s.at[slot, pl.ds(0, ref.shape[0]), pl.ds(part * PART, PART)]
            pltpu.make_async_copy(ref.at[:, pl.ds(0, PART)], dst, w_sem.at[slot, part]).wait()
        return slot

    def load(h):
        return pltpu.make_async_copy(x_ref.at[pl.ds(piece * h, piece)], a_s.at[_at(own + rows * core + piece * h, piece)], io_sem.at[h])

    load(0).start()
    load(1).start()
    table = pltpu.make_async_copy(tab_ref, sin_s, io_sem.at[2 + steps])
    table.start()
    barrier = pltpu.get_barrier_semaphore()
    for device in (partner, across, diagonal):
        pl.semaphore_signal(barrier, inc=1, device_id=(dp, device), device_id_type=MESH)

    for j in range(width // HEAD):
        gain_s[:, pl.ds(j * HEAD, HEAD)] = gain_ref[pl.ds(j, 1), :].astype(F32)
    gain = gain_s[...]

    def norm(h):
        def some(i, _):
            at = _at(own + rows * core + piece * h + 32 * i, 32)
            wide = a_s[at, :].astype(F32)
            scale = lax.rsqrt(jnp.mean(wide * wide, -1, keepdims=True) + 1e-6)
            a_s[at, :] = (wide * scale * gain).astype(BF)

        lax.fori_loop(0, piece // 32, some, None)

    def gather(k, first, count, device):
        ref = a_s.at[_at(first, count)]
        return pltpu.make_async_remote_copy(ref, ref, g_send.at[k], g_recv.at[k], device_id=(dp, device), device_id_type=MESH)

    mine, theirs = own + rows * core, own + rows * (1 - core)

    def near(h, block=mine):
        return gather(h, block + piece * h, piece, partner)

    cuts = ((0, piece), (piece, piece // 2), (piece + piece // 2, piece // 2))

    def cross(h, block=mine):
        return gather(2 + h, block + cuts[h][0], cuts[h][1], across)

    def relay(h, p):
        return gather(2 + len(cuts) + h, other + chunk * p + cuts[h][0], cuts[h][1], partner)

    def arrival(p, h):
        @pl.when(core == p)
        def _():
            cross(h, other + chunk * p).wait_recv()
            relay(h, p).start()

    for h in range(2):
        load(h).wait()
        if h == 0:
            fetch(0)
        norm(h)
        if h == 0:
            pl.semaphore_wait(barrier, 3)
        near(h).start()

        @pl.when(core == 0)
        def _():
            for k in range(len(cuts)):
                if cuts[k][0] // piece == h:
                    cross(k).start()

        if h == 0:
            for i in range(1, SLOTS):
                fetch(i)

    table.wait()
    tab = sin_s[...]
    low = lax.broadcasted_iota(jnp.int32, tab.shape, 1) < HEAD // 2
    swapped = pltpu.roll(tab, HEAD // 2, 1)
    cos_s[...] = jnp.where(low, tab, swapped)
    sin_s[...] = jnp.where(low, -swapped, tab)
    vt_s[:, HEAD:, :] = jnp.ones((groups, vt_s.shape[1] - HEAD, vt_s.shape[2]), BF)

    def turned(t, at):
        t = t.astype(BF).astype(F32)
        return (t * cos_s[at, :] + pltpu.roll(t, HEAD // 2, 1) * sin_s[at, :]).astype(BF)

    def keys_values(slot, place):
        at = _at(place, chunk)
        acc_s[0, pl.ds(0, chunk)] = _dot(a_s[at, :], w_s[slot], 1, 0)
        for g in range(groups):
            k_s[g, at, :] = turned(acc_s[0, pl.ds(0, chunk), pl.ds(g * HEAD, HEAD)], at)
            vt_s[g, pl.ds(0, HEAD), at] = acc_s[0, pl.ds(0, chunk), pl.ds(PART + g * HEAD, HEAD)].T.astype(BF)

    def queries(place, held, m, first):
        at = _at(place, m)

        def tile(n, _):
            slots = [take(first + 2 * n + b, wq_ref) for b in range(2)]
            for b in range(2):
                acc_s[b, pl.ds(0, m)] = _dot(a_s[at, :], w_s[slots[b]], 1, 0)
                fetch(first + 2 * n + b + SLOTS)
            for b in range(2):
                for h in range(per):
                    q_s[per * (2 * n + b) + h, _at(held, m), :] = turned(acc_s[b, pl.ds(0, m), pl.ds(h * HEAD, HEAD)], at)

        lax.fori_loop(0, nq // 2, tile, None)

    e = HEAD**-0.5 * LOG2E
    wide = 2 * chunk
    strips = shared // 2

    parts = [(g, i) for g in range(groups) for i in range(strips)]

    def block(b, held, j, first):
        here = _at(j * chunk, chunk)
        scores = [_dot(k_s[g, here, :], q_s[pl.ds(g * shared + 2 * i, 2), _at(held, chunk), :].reshape(wide, HEAD), 1, 1) for g, i in parts]
        if first:
            query = lax.rem(lax.broadcasted_iota(jnp.int32, (chunk, wide), 1), chunk)
            ok = query >= lax.broadcasted_iota(jnp.int32, (chunk, wide), 0)
        weights, keeps = [], []
        for (g, i), s in zip(parts, scores):
            cols = pl.ds(i * wide, wide)
            if first:
                s = jnp.where(ok, s, HIDDEN)
                top = s.max(axis=0, keepdims=True)
            else:
                old = top_s[b, g, :, cols]
                top = jnp.maximum(old, s.max(axis=0, keepdims=True))
                keeps.append(jnp.exp2((old - top) * e))
            top_s[b, g, :, cols] = top
            weights.append(jnp.exp2((s - top) * e).astype(BF))
        for k, ((g, i), w) in enumerate(zip(parts, weights)):
            cols = pl.ds(i * wide, wide)
            new = _dot(vt_s[g, :, here], w, 1, 0)
            mix_s[b, g, :, cols] = new if first else mix_s[b, g, :, cols] * keeps[k] + new

    def finish(b, seen):
        for k in range(groups * shared):
            g, cols = k // shared, pl.ds(k % shared * chunk, chunk)
            out = mix_s[b, g, pl.ds(0, HEAD), cols] * (1 / mix_s[b, g, pl.ds(HEAD, 1), cols])
            seen_s[_at(seen, chunk), pl.ds(k * HEAD, HEAD)] = out.T.astype(BF)

    def pair(p, n):
        return pltpu.make_async_remote_copy(dsend_s.at[n, pl.ds(p * piece, piece)], drecv_s.at[p, n], d_send.at[p, n], d_recv.at[p, n],
                                            device_id=(dp, partner), device_id_type=MESH)

    def link(p, n, source, device):
        return pltpu.make_async_remote_copy(drecv_s.at[p, n], xrecv_s.at[source, n], x_send.at[p, n], x_recv.at[source, n],
                                            device_id=(dp, device), device_id_type=MESH)

    def swap(n):
        dst = a_s.at[pl.ds(0, rows), _at(n * 2 * TILE, 2 * TILE)]
        return pltpu.make_async_remote_copy(dsend_s.at[n], dst, o_send.at[n], o_recv.at[n], device_id=(dp, partner), device_id_type=MESH)

    slot = take(0, wq_ref)

    def local(i, _):
        @pl.when(i == 1)
        def _():
            for h in range(2):
                near(h, theirs).wait_recv()

        keys_values(slot, jnp.where(i == 0, mine, theirs))

    lax.fori_loop(0, 2, local, None)
    fetch(SLOTS)
    queries(own, 0, half, 1)
    arrival(0, 0)

    def inner(i, _):
        first = lax.div(own, chunk)
        block(i, i * chunk, first + i, True)

        @pl.when((i == 1) & (core == 1))
        def _():
            for h in range(len(cuts)):
                cross(h).start()

        @pl.when(i == 1)
        def _():
            for h in range(1, len(cuts)):
                arrival(0, h)

        lax.fori_loop(0, i, lambda j, _: block(i, i * chunk, first + j, False), None)

    lax.fori_loop(0, 2, inner, None)

    def add(p, n):
        pair(p, n).wait_recv()
        drecv_s[p, n] = (part_s[lax.rem(n, 2)] + drecv_s[p, n].astype(F32)).astype(BF)

    def send(p, n):
        link(p, n, core, 2 * (1 - chip) + p).start()

    def arrived(p, _):
        place = other + chunk * p
        first = np_ + nc * p

        @pl.when(core != p)
        def _():
            for h in range(len(cuts)):
                relay(h, p).wait_recv()

        slot = take(first, wq_ref)
        keys_values(slot, place)
        fetch(first + SLOTS)
        queries(place, half, chunk, first + 1)
        whole = lax.div(place, chunk)

        block(2, half, whole, True)
        lax.fori_loop(0, whole, lambda j, _: block(2, half, j, False), None)
        finish(2, jnp.int32(0))

        @pl.when(p == 1)
        def _():
            add(p - 1, jnp.int32(steps - 1))
            send(p - 1, jnp.int32(steps - 1))
            for h in range(2):
                near(h).wait_send()
            for h in range(len(cuts)):
                cross(h).wait_send()
                relay(h, core).wait_send()

        def tile(n, _):
            slots = [take(first + np_ + 2 * n + b, wo_ref) for b in range(2)]
            pl.when((p == 0) & (n == 0))(lambda: arrival(1, 0))

            @pl.when((p == 0) & (n == steps - 2))
            def _():
                for m in range(steps - 3):
                    send(p, jnp.int32(m))

            @pl.when((p == 0) & (n == steps - 1))
            def _():
                for h in range(1, len(cuts)):
                    arrival(1, h)

            for b in range(2):
                acc_s[b, pl.ds(0, chunk)] = _dot(seen_s[pl.ds(0, chunk)], w_s[slots[b], pl.ds(0, depth)], 1, 0)
                fetch(first + np_ + 2 * n + b + SLOTS)
            for b in range(2):
                cols = pl.ds(b * TILE, TILE)
                dsend_s[n, _at(p * piece, piece), cols] = acc_s[b, _at(piece * (1 - core), piece)].astype(BF)
                part_s[lax.rem(n, 2), :, cols] = acc_s[b, _at(piece * core, piece)]
            pair(p, n).start()
            pl.when(n > 0)(lambda: add(p, n - 1))
            pl.when((n > 0) & ((p == 1) | (n >= steps - 2)))(lambda: send(p, n - 1))

            def outer(i, _):
                block(i, i * chunk, p, False)

            lax.fori_loop(0, jnp.where((chip == 1) & (n == 1), 2, 0), outer, None)

        lax.fori_loop(0, steps, tile, None)

    lax.fori_loop(0, 2, arrived, None)

    lax.fori_loop(0, 2, lambda i, _: finish(i, i * chunk), None)
    add(1, jnp.int32(steps - 1))
    send(1, jnp.int32(steps - 1))
    wides = mix_s.shape[3] // TILE

    def kept(n, b, h):
        k = (2 * n + b) * 2 + h
        s = lax.div(k, wides)
        return lax.div(s, groups), lax.rem(s, groups), pl.ds(0, piece), _at(lax.rem(k, wides) * TILE, TILE)

    again = pltpu.make_async_copy(x_ref, a_s.at[pl.ds(rows, rows)], io_sem.at[0])
    again.start()

    def last(n, _):
        first = np_ + 2 * nc + 2 * n
        slots = [take(first + b, wo_ref) for b in range(2)]
        for p in range(2):
            pair(p, n).wait_send()
        for b in range(2):
            acc_s[b] = _dot(seen_s[...], w_s[slots[b], pl.ds(0, depth)], 1, 0)
        for b in range(2):
            dsend_s[n, :, pl.ds(b * TILE, TILE)] = acc_s[b, _at(rows * (1 - core), rows)].astype(BF)
            for h in range(2):
                mix_s[kept(n, b, h)] = acc_s[b, _at(rows * core + piece * h, piece)]
        swap(n).start()
        for b in range(2):
            fetch(first + b + SLOTS)

    lax.fori_loop(0, steps, last, None)

    def store(n):
        cols = _at(n * 2 * TILE, 2 * TILE)
        return pltpu.make_async_copy(a_s.at[pl.ds(rows, rows), cols], y_ref.at[:, cols], io_sem.at[2 + n])

    def close(n, _):
        swap(n).wait_recv()
        for source in range(2):
            link(0, n, source, across).wait_recv()
        for b in range(2):
            cols = _at((2 * n + b) * TILE, TILE)
            for source in range(2):
                at = pl.ds(source * piece, piece)
                summed = mix_s[kept(n, b, source)] + a_s[at, cols].astype(F32) + xrecv_s[source, n, :, pl.ds(b * TILE, TILE)].astype(F32)
                to = pl.ds(rows + source * piece, piece)
                a_s[to, cols] = (a_s[to, cols].astype(F32) + summed).astype(BF)
        store(n).start()

    again.wait()
    lax.fori_loop(0, steps, close, None)

    def sent(n, _):
        for p in range(2):
            link(p, n, core, across).wait_send()
        swap(n).wait_send()
        store(n).wait()

    lax.fori_loop(0, steps, sent, None)


def _table(tokens):
    half = HEAD // 2
    power = np.float32(THETA) ** (-np.arange(half, dtype=np.float32) / np.float32(half))
    angle = np.arange(tokens, dtype=np.float32)[:, None] * power.astype(np.float32)
    return np.concatenate([np.cos(angle), np.sin(angle)], 1).astype(np.float32)


def solution(mesh):
    group = mesh.shape["tp"]

    def step(x, gain, wq, wk, wv, wo):
        rows, width = x.shape
        tokens, piece = rows * group, rows // 2
        heads, groups = wq.shape[1] // HEAD, wk.shape[1] // HEAD
        depth, steps = wo.shape[0], width // TILE // 2
        dma = pltpu.SemaphoreType.DMA
        vmem, hbm = pl.BlockSpec(memory_space=pltpu.VMEM), pl.BlockSpec(memory_space=pltpu.HBM)
        cols = heads // groups * rows
        return pl.pallas_call(
            _whole,
            out_shape=jax.ShapeDtypeStruct((rows, width), BF),
            in_specs=[hbm, vmem, hbm, hbm, hbm, hbm, hbm],
            out_specs=hbm,
            scratch_shapes=[
                pltpu.VMEM((1, width), F32),
                pltpu.VMEM((tokens, width), BF),
                pltpu.VMEM((tokens, HEAD), F32),
                pltpu.VMEM((tokens, HEAD), F32),
                pltpu.VMEM((heads, 3 * rows, HEAD), BF),
                pltpu.VMEM((groups, tokens, HEAD), BF),
                pltpu.VMEM((groups, HEAD + 8, tokens), BF),
                pltpu.VMEM((2 * rows, depth), BF),
                pltpu.VMEM((2, 2 * rows, TILE), F32),
                pltpu.VMEM((3, groups, 1, cols), F32),
                pltpu.VMEM((3, groups, HEAD + 8, cols), F32),
                pltpu.VMEM((SLOTS, width, TILE), BF),
                pltpu.VMEM((2, piece, 2 * TILE), F32),
                pltpu.VMEM((steps, rows, 2 * TILE), BF),
                pltpu.VMEM((2, steps, piece, 2 * TILE), BF),
                pltpu.VMEM((2, steps, piece, 2 * TILE), BF),
                dma((SLOTS, 2)), dma((3 + steps,)), dma((8,)), dma((8,)), dma((2, steps)), dma((2, steps)), dma((2, steps)), dma((2, steps)),
                dma((steps,)), dma((steps,)),
            ],
            compiler_params=pltpu.CompilerParams(collective_id=0, has_side_effects=True, vmem_limit_bytes=VMEM),
            cost_estimate=pl.CostEstimate(flops=2 * tokens * width * (2 * depth + 2 * groups * HEAD) + 2 * heads * tokens * tokens * HEAD,
                                          transcendentals=heads * tokens * tokens // 2,
                                          bytes_accessed=3 * 2 * width * (2 * depth + 2 * groups * HEAD)),
        )(x, gain.reshape(width // HEAD, HEAD), jnp.asarray(_table(tokens)), wq, wk, wv, wo)

    tokens, columns = P(("dp", "tp"), None), P(None, "tp")
    return jax.shard_map(
        step,
        mesh=mesh,
        in_specs=(tokens, P(None), columns, columns, columns, P("tp", None)),
        out_specs=tokens,
        check_vma=False,
    )
```
